64 devices in a mesh: rep: 8 (over x, y, core), dp: 8 (over z).
Axes of the slice: x: 2, y: 2, z: 8, core: 2. Of those that a mesh axis runs over, the one named last changes fastest.
The devices are a block of a 4x4x8 slice.
Arguments:
- x: bfloat16 [64, 4096, 512], P(('rep', 'dp')), parts along dimension 0
- dy: bfloat16 [64, 4096, 512], P(('rep', 'dp')), parts along dimension 0
- w_gate: bfloat16 [2, 512, 1280], P(None, 'dp')
- w_up: bfloat16 [2, 512, 1280], P(None, 'dp')
- w_down: bfloat16 [2, 1280, 512], P(None, 'dp')
- m_w_gate: float32 [2, 512, 1280], P(None, 'dp')
- m_w_up: float32 [2, 512, 1280], P(None, 'dp')
- m_w_down: float32 [2, 1280, 512], P(None, 'dp')
- v_w_gate: float32 [2, 512, 1280], P(None, 'dp')
- v_w_up: float32 [2, 512, 1280], P(None, 'dp')
- v_w_down: float32 [2, 1280, 512], P(None, 'dp')
Outputs:
- output 1: bfloat16 [16, 512, 1280], P('rep', 'dp'), parts along dimension 0
- output 2: bfloat16 [16, 512, 1280], P('rep', 'dp'), parts along dimension 0
- output 3: bfloat16 [16, 1280, 512], P('rep', 'dp'), parts along dimension 0
- output 4: float32 [16, 512, 1280], P('rep', 'dp'), parts along dimension 0
- output 5: float32 [16, 512, 1280], P('rep', 'dp'), parts along dimension 0
- output 6: float32 [16, 1280, 512], P('rep', 'dp'), parts along dimension 0
- output 7: float32 [16, 512, 1280], P('rep', 'dp'), parts along dimension 0
- output 8: float32 [16, 512, 1280], P('rep', 'dp'), parts along dimension 0
- output 9: float32 [16, 1280, 512], P('rep', 'dp'), parts along dimension 0
There are 8 independent parts. The reference program is written for one: setup_inputs(seed, part) draws one part's arguments, and reference() takes and returns one part's arrays. A program takes and returns all parts, laid end to end along the dimension named above; an argument that names none is the same for every part.
All inputs are finite; a program needn't handle non-finite values.
Results may differ from the reference program's by a relative error of at most 0.022.
Values are sent between devices in bfloat16 or wider.
A program may use at most 768 MiB of HBM per device.

```python
import jax
import jax.numpy as jnp
from jax import lax

SEQUENCES = 8
TOKENS = 4096
D = 512
FF = 1280
LAYERS = 2
NAMES = ("w_gate", "w_up", "w_down")
SHAPES = {"w_gate": (LAYERS, D, FF), "w_up": (LAYERS, D, FF), "w_down": (LAYERS, FF, D)}


def bump(key, n, height):
    away = (jnp.arange(n, dtype=jnp.int32) - jax.random.randint(key, (), 0, n, jnp.int32)) % n
    return jnp.where(away < n // 8, height, 1.0)


def together(key, own, strength):
    shared = jax.random.normal(key, own.shape[1:], jnp.float32)
    return (own + strength * shared) * lax.rsqrt(1 + strength * strength)


def setup_inputs(seed: int = 0, part: int = 0) -> dict:
    kx, kdy, ka, kb, kz, kf, kh, kl, *keys = jax.random.split(jax.random.key(seed), 8 + 3 * len(NAMES))
    kx, kdy, ka, kb = (jax.random.fold_in(k, part) for k in (kx, kdy, ka, kb))
    kw, km, kv = (keys[i::3] for i in range(3))
    shape = (SEQUENCES, TOKENS, D)
    much_x, much_dy = jax.random.uniform(kz, (2,), jnp.float32, 0.0, 1.0)
    loud = 2.0 ** jax.random.uniform(jax.random.fold_in(kz, 1), (), jnp.float32, -1.0, 2.0)
    layers = 2.0 ** jax.random.uniform(kl, (LAYERS, 1, 1), jnp.float32, -1.0, 1.0)
    x = together(ka, jax.random.normal(kx, shape, jnp.float32), much_x) * bump(kf, D, 4.0)
    dy = together(kb, jax.random.normal(kdy, shape, jnp.float32), much_dy)
    drawn = {"x": x.astype(jnp.bfloat16), "dy": (loud * dy * (SEQUENCES * TOKENS) ** -0.5).astype(jnp.bfloat16)}
    for key, name in zip(kw, NAMES, strict=True):
        w = jax.random.normal(key, SHAPES[name], jnp.float32) * SHAPES[name][1] ** -0.5
        drawn[name] = (w * {"w_gate": 1.0, "w_up": bump(kh, FF, 4.0), "w_down": layers}[name]).astype(jnp.bfloat16)
    for key, name in zip(km, NAMES, strict=True):
        drawn[f"m_{name}"] = 0.1 * jax.random.normal(key, SHAPES[name], jnp.float32)
    for key, name in zip(kv, NAMES, strict=True):
        drawn[f"v_{name}"] = jax.random.uniform(key, SHAPES[name], jnp.float32, 0.005, 0.015)
    return drawn


def matmul(a, w):
    return jnp.dot(a, w, preferred_element_type=jnp.float32).astype(jnp.bfloat16)


def normed(h):
    wide = h.astype(jnp.float32)
    scale = lax.rsqrt(jnp.mean(wide**2, -1, keepdims=True) + 1e-6)
    return (wide * scale).astype(jnp.bfloat16)


def layer(h, w):
    a = normed(h)
    gate = jnp.dot(a, w["w_gate"], preferred_element_type=jnp.float32)
    up = jnp.dot(a, w["w_up"], preferred_element_type=jnp.float32)
    return h + matmul((jax.nn.silu(gate) * up).astype(jnp.bfloat16), w["w_down"])


def adamw(w, m, v, g):
    m = 0.9 * m + 0.1 * g
    v = 0.95 * v + 0.05 * g * g
    step = m * lax.rsqrt(v + 1e-8) + 0.1 * w
    return (w - 0.02 * step).astype(jnp.bfloat16), m, v


def clipped(gradients, sum_of_squares, count):
    factor = jnp.minimum(1.0, 0.5 * lax.rsqrt(sum_of_squares / count + 1e-30))
    return [g * factor for g in gradients]


def stack(weights, h):
    return lax.scan(lambda h, w: (layer(h, w), None), h, weights)[0]


def reference(x, dy, w_gate, w_up, w_down, m_w_gate, m_w_up, m_w_down, v_w_gate, v_w_up, v_w_down):
    weights = dict(zip(NAMES, (w_gate, w_up, w_down), strict=True))

    def take(so_far, sequence):
        h, by_y = sequence
        _, back = jax.vjp(lambda w: stack(w, h), weights)
        return jax.tree.map(lambda total, term: total + term.astype(jnp.float32), so_far, back(by_y)[0]), None

    none_yet = {name: jnp.zeros(w.shape, jnp.float32) for name, w in weights.items()}
    by_weights, _ = lax.scan(take, none_yet, (x, dy))
    gradients = [by_weights[name].astype(jnp.bfloat16).astype(jnp.float32) for name in NAMES]
    gradients = clipped(gradients, sum(jnp.sum(g * g) for g in gradients), sum(g.size for g in gradients))
    new = [
        adamw(w.astype(jnp.float32), m, v, g)
        for w, m, v, g in zip((w_gate, w_up, w_down), (m_w_gate, m_w_up, m_w_down), (v_w_gate, v_w_up, v_w_down), gradients, strict=True)
    ]
    return tuple(one[which] for which in range(3) for one in new)
```

```python
import functools

import jax
import jax.numpy as jnp
from jax import lax
from jax.experimental import pallas as pl
from jax.experimental.pallas import tpu as pltpu
from jax.sharding import PartitionSpec as P

BF, F32 = jnp.bfloat16, jnp.float32
C = 256
TILES = 4
A, B = 0, 1
RIGHT, LEFT = 0, 1


def dot(a, b, ca=1, cb=0):
    return lax.dot_general(a, b, (((ca,), (cb,)), ((), ())), preferred_element_type=F32)


def sigmoid(g):
    return 0.5 * jnp.tanh(0.5 * g) + 0.5


def normed(h):
    return (h * lax.rsqrt(jnp.mean(h * h, -1, keepdims=True) + 1e-6)).astype(BF)


def when(condition):
    return (lambda body: body()) if condition is True else pl.when(condition)


def routes(n):
    far, near = n // 2, n - 1 - n // 2
    hops = {(A, RIGHT): far, (A, LEFT): near, (B, RIGHT): near, (B, LEFT): far}
    number, k = {}, 0
    for (m, d), count in hops.items():
        for hop in range(1, count + 1):
            number[m, d, hop] = k
            k += 1
    return hops, number, k


def step_kernel(
    n, layers, d_model, ff, tokens,
    x_hbm, dy_hbm, wg_hbm, wu_hbm, wd_hbm,
    gg_ref, gu_ref, gd_ref, squares_ref, a_hbm,
    x, a, dy, da, hidden, wgu, wd, dgu, hid, acc, dwd, buf, bufd, ss, ssd, others,
    local_sem, own_sem, ag_recv, ag_send, pair_recv, pair_send, rs_recv, rs_send, rsd_recv, rsd_send, sq_recv, sq_send, credit,
):
    me, rep = lax.axis_index("dp"), lax.axis_index("rep")
    core = lax.rem(rep, 2)
    partner = {"rep": rep + 1 - 2 * core}
    ring = lambda off: lax.rem(me + off + n, n)
    to = {RIGHT: {"dp": ring(1)}, LEFT: {"dp": ring(-1)}}
    sign = {RIGHT: 1, LEFT: -1}
    hops, number, messages = routes(n)
    far = n // 2
    chunks = ff // C
    rows_gu, rows_d = d_model // n, ff // n
    half_gu, half_d = rows_gu // 2, rows_d // 2
    half_w = d_model // 2
    tile = tokens // TILES
    MESH = pl.DeviceIdType.MESH

    barrier = pltpu.get_barrier_semaphore()
    for off in range(1, n):
        pl.semaphore_signal(barrier, inc=1, device_id={"dp": ring(off)}, device_id_type=MESH)
    pl.semaphore_signal(barrier, inc=1, device_id=partner, device_id_type=MESH)
    mine_gu = pl.ds(pl.multiple_of(me * rows_gu, rows_gu), rows_gu)
    mine_d = pl.ds(pl.multiple_of(me * rows_d, rows_d), rows_d)
    own = []
    for l in range(layers):
        for c in range(chunks):
            for m, src in ((0, wg_hbm), (1, wu_hbm)):
                own.append((src.at[l, :, pl.ds(c * C, C)], wgu.at[l, c, mine_gu, pl.ds(m * C, C)]))
        own.append((wd_hbm.at[l], wd.at[l, mine_d]))
    own = [pltpu.make_async_copy(s, t, own_sem.at[i]) for i, (s, t) in enumerate(own)]
    for copy in own:
        copy.start()
    load_x = pltpu.make_async_copy(x_hbm, x, local_sem.at[0])
    load_dy = pltpu.make_async_copy(dy_hbm, dy, local_sem.at[1])
    load_x.start()
    load_dy.start()
    pl.semaphore_wait(barrier, n)
    for copy in own:
        copy.wait()

    units = [(0, 0, 1), (0, 1, 2), (0, 3, chunks - 3), (0, None, None), (1, 0, 3), (1, 3, chunks - 3), (1, None, None)]

    def piece(u, m, owner):
        l, c, count = units[u]
        if c is None:
            return wd.at[l, pl.ds(pl.multiple_of(owner * rows_d + core * half_d, half_d), half_d), pl.ds(m * half_w, half_w)]
        return wgu.at[l, pl.ds(c, count), pl.ds(pl.multiple_of(owner * rows_gu + core * half_gu, half_gu), half_gu), pl.ds(m * C, C)]

    def everything(u):
        l, c, count = units[u]
        if c is None:
            return wd.at[l, pl.ds(0, messages * half_d), pl.ds(0, half_w)]
        return wgu.at[l, pl.ds(c, count), pl.ds(0, messages * half_gu), pl.ds(0, C)]

    def gather(u, k):
        for (m, d), count in hops.items():
            if k > count:
                continue
            block = piece(u, m, ring(-sign[d] * k))
            if k:
                pltpu.make_async_copy(block, block, ag_recv.at[u, number[m, d, k]]).wait()
            if k < count:
                pltpu.make_async_remote_copy(
                    src_ref=block, dst_ref=block, send_sem=ag_send.at[u], recv_sem=ag_recv.at[u, number[m, d, k + 1]],
                    device_id=to[d], device_id_type=MESH,
                ).start()
            if k:
                pltpu.make_async_remote_copy(
                    src_ref=block, dst_ref=block, send_sem=pair_send.at[u], recv_sem=pair_recv.at[u],
                    device_id=partner, device_id_type=MESH,
                ).start()

    def gathered(u):
        pltpu.make_async_copy(everything(u), everything(u), pair_recv.at[u]).wait()

    def rs_parts(down, s):
        if down:
            l = s
            return rows_d, half_w, dwd.at[l], bufd.at[l], rsd_recv, rsd_send.at[l], l
        slot = lax.rem(s, 2)
        return rows_gu, C, acc.at[slot], buf.at[slot], rs_recv, rs_send.at[slot], slot

    def rs_step(down, s, k, wait_credit=None):
        rows, width, total, slots, recv, send, slot = rs_parts(down, s)
        if k == 0 and wait_credit is not None:

            @when(wait_credit)
            def _():
                pl.semaphore_wait(credit.at[0], 1)
                pl.semaphore_wait(credit.at[1], 1)

        out = []
        for i, ((m, d), count) in enumerate(hops.items()):
            if k >= count:
                continue
            owner = ring(sign[d] * (count - k))
            term = total[pl.ds(pl.multiple_of(owner * rows, rows), rows), pl.ds(m * width, width)]
            if k == 0:
                at = messages + i
            else:
                at = number[m, d, k]
                pltpu.make_async_copy(slots.at[at], slots.at[at], recv.at[slot, at]).wait()
                term = term + slots[at].astype(F32)
            slots[at] = term.astype(BF)
            out.append((m, d, at))
        for m, d, at in out:
            there = number[m, d, k + 1]
            pltpu.make_async_remote_copy(
                src_ref=slots.at[at], dst_ref=slots.at[there], send_sem=send, recv_sem=recv.at[slot, there],
                device_id=to[d], device_id_type=MESH,
            ).start()

    def rs_final(down, s, l, c, give=None):
        rows, width, total, slots, recv, send, slot = rs_parts(down, s)
        sums = ssd if down else ss
        for m in (A, B):
            g = total[pl.ds(pl.multiple_of(me * rows, rows), rows), pl.ds(m * width, width)]
            for d in (RIGHT, LEFT):
                at = number[m, d, hops[m, d]]
                pltpu.make_async_copy(slots.at[at], slots.at[at], recv.at[slot, at]).wait()
                g = g + slots[at].astype(F32)
            g = g.astype(BF)
            if down:
                gd_ref[l, :, pl.ds(m * width, width)] = g
            else:
                (gg_ref, gu_ref)[m][l, :, pl.ds(pl.multiple_of(c * C, C), C)] = g
            wide = g.astype(F32)
            sums[...] += wide * wide
        pltpu.make_async_copy(slots.at[pl.ds(0, messages)], slots.at[pl.ds(0, messages)], send).wait()
        if give is not None:

            @when(give)
            def _():
                pl.semaphore_signal(credit.at[0], inc=1, device_id=to[LEFT], device_id_type=MESH)
                pl.semaphore_signal(credit.at[1], inc=1, device_id=to[RIGHT], device_id_type=MESH)

    def tile_rows(t):
        return pl.ds(pl.multiple_of(t * tile, tile), tile)

    gather(0, 0)
    gather(1, 0)
    ss[...] = jnp.zeros_like(ss)
    ssd[...] = jnp.zeros_like(ssd)
    load_x.wait()

    def first_norm(lo, hi):
        @pl.loop(lo, hi)
        def _(t):
            r = tile_rows(t)
            a[r] = normed(x[r].astype(F32))

    first_norm(0, 2)
    gather(0, 1)
    gather(1, 1)
    gather(2, 0)
    first_norm(2, 4)
    save_a = pltpu.make_async_copy(a, a_hbm, local_sem.at[2])
    save_a.start()
    gather(0, 2)
    gather(1, 2)
    gather(2, 1)
    da[...] = jnp.zeros_like(da)
    gather(0, 3)
    gather(1, 3)
    gather(2, 2)
    load_dy.wait()
    gather(0, 4)
    gathered(0)

    before = {
        1: [(1, 4), (2, 3), (3, 0)],
        2: [(3, 1), (4, 0)],
        3: [(2, 4), (3, 2), (4, 1), (5, 0)],
        4: [(3, 3), (4, 2), (5, 1), (6, 0)],
    }
    ready = {1: 1, 3: 2}
    for c in range(chunks):
        for event in before.get(c, ()):
            gather(*event)
        if c in ready:
            gathered(ready[c])

        @pl.loop(0, TILES)
        def _(t):
            r = tile_rows(t)
            both = dot(a[r], wgu[0, c])
            g, u = both[:, :C], both[:, C:]
            hidden[r, c * C : (c + 1) * C] = (g * sigmoid(g) * u).astype(BF)

    for event in ((3, 4), (4, 3), (5, 2), (6, 1)):
        gather(*event)
    gathered(3)
    save_a.wait()
    between = {0: [], 1: [(4, 4), (5, 3), (6, 2)], 2: [(5, 4), (6, 3)], 3: [(6, 4)]}
    for t in range(TILES):
        for event in between[t]:
            gather(*event)
        r = pl.ds(t * tile, tile)
        out = dot(hidden[r], wd[0]).astype(BF)
        h = (x[r].astype(F32) + out.astype(F32)).astype(BF)
        x[r] = h
        a[r] = normed(h.astype(F32))
    for u in (4, 5, 6):
        gathered(u)

    def first_half(l, c, t, back):
        r = tile_rows(t)
        both = dot(a[r], wgu[l, c])
        g, u = both[:, :C], both[:, C:]
        wdc = wd[l, pl.ds(pl.multiple_of(c * C, C), C)]
        dh = dot(back[r], wdc, 1, 1).astype(BF).astype(F32)
        s = sigmoid(g)
        silu = g * s
        slope = s + silu * (1.0 - s)
        both = jnp.concatenate([(dh * u * slope).astype(BF), (dh * silu).astype(BF)], axis=1)
        dgu[r] = both
        if l == layers - 1:
            hid[r] = (silu * u).astype(BF)
            da[r] += dot(both, wgu[l, c], 1, 1)

    last = layers - 1

    @pl.loop(0, chunks)
    def _(c):
        first_half_1 = functools.partial(first_half, last, c, back=dy)

        @pl.when(c >= 1)
        def _():
            rs_step(False, c - 1, 0, c >= 3)

        @pl.when(c >= 2)
        def _():
            rs_step(False, c - 2, 3)

        first_half_1(t=0)
        first_half_1(t=1)

        @pl.when(c >= 1)
        def _():
            rs_step(False, c - 1, 1)

        @pl.when(c >= 2)
        def _():
            rs_final(False, c - 2, last, c - 2, c >= 0)

        first_half_1(t=2)
        first_half_1(t=3)

        @pl.when(c >= 1)
        def _():
            rs_step(False, c - 1, 2)

        acc[lax.rem(c, 2)] = dot(a[...], dgu[...], 0, 0)
        dwd[last, pl.ds(pl.multiple_of(c * C, C), C)] = dot(hid[...], dy[...], 0, 0)

    load_a = pltpu.make_async_copy(a_hbm, a, local_sem.at[2])
    load_a.start()
    rs_step(False, chunks - 1, 0, True)
    rs_step(False, chunks - 2, 3)
    rs_step(True, last, 0)

    def norm_back(lo, hi):
        @pl.loop(lo, hi)
        def _(t):
            r = tile_rows(t)
            h = x[r].astype(F32)
            by_a = da[r].astype(BF).astype(F32)
            scale = lax.rsqrt(jnp.mean(h * h, -1, keepdims=True) + 1e-6)
            along = jnp.mean(h * by_a, -1, keepdims=True) * (scale * scale * scale)
            by_h = (by_a * scale - h * along).astype(BF)
            x[r] = (dy[r].astype(F32) + by_h.astype(F32)).astype(BF)

    norm_back(0, 2)
    rs_step(False, chunks - 1, 1)
    rs_final(False, chunks - 2, last, chunks - 2, True)
    norm_back(2, 4)
    rs_step(False, chunks - 1, 2)

    @pl.loop(0, chunks)
    def _(c):
        cols = pl.ds(pl.multiple_of(c * C, C), C)
        dwd[0, cols] = dot(hidden[:, cols], x[...], 0, 0)

    load_a.wait()

    @pl.loop(0, chunks)
    def _(c):
        half_0 = functools.partial(first_half, 0, c, back=x)

        @pl.when(c >= 1)
        def _():
            rs_step(False, chunks + c - 1, 0, c >= 1)

        @pl.when(c >= 2)
        def _():
            rs_step(False, chunks + c - 2, 3)

        @pl.when(c == 0)
        def _():
            rs_step(False, chunks - 1, 3)
            rs_step(True, 0, 0)

        half_0(t=0)

        @pl.when(c == 0)
        def _():
            rs_step(True, last, 1)

        @pl.when(c == 1)
        def _():
            rs_step(True, last, 3)

        @pl.when(c == 2)
        def _():
            rs_step(True, 0, 2)

        half_0(t=1)

        @pl.when(c >= 1)
        def _():
            rs_step(False, chunks + c - 1, 1)

        @pl.when(c >= 2)
        def _():
            rs_final(False, chunks + c - 2, 0, c - 2, c - 2 <= chunks - 3)

        @pl.when(c == 0)
        def _():
            rs_final(False, chunks - 1, last, chunks - 1, True)

        half_0(t=2)

        @pl.when(c == 1)
        def _():
            rs_step(True, 0, 1)

        @pl.when(c == 2)
        def _():
            rs_final(True, last, last, None)

        @pl.when(c == 3)
        def _():
            rs_step(True, 0, 3)

        half_0(t=3)

        @pl.when(c == 0)
        def _():
            rs_step(True, last, 2)

        @pl.when(c == 4)
        def _():
            rs_final(True, 0, 0, None)

        @pl.when(c >= 1)
        def _():
            rs_step(False, chunks + c - 1, 2)

        acc[lax.rem(chunks + c, 2)] = dot(a[...], dgu[...], 0, 0)

    s = 2 * chunks - 1
    rs_step(False, s, 0, True)
    rs_step(False, s - 1, 3)
    rs_step(False, s, 1)
    rs_final(False, s - 1, 0, chunks - 2)
    rs_step(False, s, 2)
    rs_step(False, s, 3)
    rs_final(False, s, 0, chunks - 1)

    total = jnp.sum(ss[...]) + jnp.sum(ssd[...])
    others[me] = jnp.full(others.shape[1:], total, F32)
    copies = []
    for off in range(1, n):
        copies.append(
            pltpu.make_async_remote_copy(
                src_ref=others.at[me], dst_ref=others.at[me], send_sem=sq_send.at[off], recv_sem=sq_recv.at[off],
                device_id={"dp": ring(off)}, device_id_type=MESH,
            )
        )
    for copy in copies:
        copy.start()
    for off in range(1, n):
        slot = others.at[ring(-off)]
        pltpu.make_async_copy(slot, slot, sq_recv.at[off]).wait()
    squares_ref[...] = jnp.sum(others[...], axis=0)
    for copy in copies:
        copy.wait_send()
    for u in range(len(units)):
        pltpu.make_async_copy(everything(u), everything(u), ag_send.at[u]).wait()
        pltpu.make_async_copy(everything(u), everything(u), pair_send.at[u]).wait()


def adamw_kernel(count, squares, *refs):
    factor = jnp.minimum(1.0, 0.5 * lax.rsqrt(squares[0:1, 0:1] / count + 1e-30))
    gs, ws, ms, vs, new_w, new_m, new_v = (refs[i : i + 3] for i in range(0, 21, 3))
    for i in range(3):
        g = gs[i][...].astype(F32) * factor
        m = 0.9 * ms[i][...] + 0.1 * g
        v = 0.95 * vs[i][...] + 0.05 * g * g
        w = ws[i][...].astype(F32)
        new_w[i][...] = (w - 0.02 * (m * lax.rsqrt(v + 1e-8) + 0.1 * w)).astype(BF)
        new_m[i][...] = m
        new_v[i][...] = v


def solution(mesh):
    n = mesh.shape["dp"]

    def step(x, dy, *arrays):
        weights, m, v = (arrays[i : i + 3] for i in (0, 3, 6))
        x, dy = x[0], dy[0]
        tokens, d_model = x.shape
        layers, rows_gu, ff = weights[0].shape
        rows_d = weights[2].shape[1]
        chunks = ff // C
        messages = 2 * (n - 1)
        hbm = pl.BlockSpec(memory_space=pl.ANY)
        vmem = pl.BlockSpec(memory_space=pltpu.VMEM)
        dma = pltpu.SemaphoreType.DMA
        gg, gu, gd, squares, _ = pl.pallas_call(
            functools.partial(step_kernel, n, layers, d_model, ff, tokens),
            out_shape=[jax.ShapeDtypeStruct(w.shape, BF) for w in weights]
            + [jax.ShapeDtypeStruct((8, 128), F32), jax.ShapeDtypeStruct((tokens, d_model), BF)],
            in_specs=[hbm] * 5,
            out_specs=[vmem] * 4 + [hbm],
            scratch_shapes=[
                pltpu.VMEM((tokens, d_model), BF),
                pltpu.VMEM((tokens, d_model), BF),
                pltpu.VMEM((tokens, d_model), BF),
                pltpu.VMEM((tokens, d_model), F32),
                pltpu.VMEM((tokens, ff), BF),
                pltpu.VMEM((layers, chunks, d_model, 2 * C), BF),
                pltpu.VMEM((layers, ff, d_model), BF),
                pltpu.VMEM((tokens, 2 * C), BF),
                pltpu.VMEM((tokens, C), BF),
                pltpu.VMEM((2, d_model, 2 * C), F32),
                pltpu.VMEM((layers, ff, d_model), F32),
                pltpu.VMEM((2, messages + 4, rows_gu, C), BF),
                pltpu.VMEM((layers, messages + 4, rows_d, d_model // 2), BF),
                pltpu.VMEM((rows_gu, C), F32),
                pltpu.VMEM((rows_d, d_model // 2), F32),
                pltpu.VMEM((n, 8, 128), F32),
                dma((3,)),
                dma((layers * (2 * chunks + 1),)),
                dma((7, messages)),
                dma((7,)),
                dma((7,)),
                dma((7,)),
                dma((2, messages)),
                dma((2,)),
                dma((layers, messages)),
                dma((layers,)),
                dma((n,)),
                dma((n,)),
                pltpu.SemaphoreType.REGULAR((2,)),
            ],
            compiler_params=pltpu.CompilerParams(collective_id=0, has_side_effects=True, vmem_limit_bytes=67043328),
            name="train_step",
        )(x, dy, *weights)

        cut = 2
        specs = [pl.BlockSpec((1, w.shape[1] // cut, w.shape[2]), lambda l, i: (l, i, 0)) for w in weights]
        out = pl.pallas_call(
            functools.partial(adamw_kernel, float(n * sum(w.size for w in weights))),
            grid=(layers, cut),
            out_shape=[jax.ShapeDtypeStruct(w.shape, dtype) for dtype in (BF, F32, F32) for w in weights],
            in_specs=[pl.BlockSpec((8, 128), lambda l, i: (0, 0))] + specs * 4,
            out_specs=specs * 3,
            name="adamw",
        )(squares, gg, gu, gd, *weights, *m, *v)
        return tuple(out)

    states, cut = P(("rep", "dp"), None, None), P(None, "dp", None)
    return jax.shard_map(
        step,
        mesh=mesh,
        in_specs=(states, states) + (cut,) * 9,
        out_specs=(P("rep", "dp", None),) * 9,
        check_vma=False,
    )
```

```python
import functools

import jax
import jax.numpy as jnp
from jax import lax
from jax.experimental import pallas as pl
from jax.experimental.pallas import tpu as pltpu
from jax.sharding import PartitionSpec as P

BF, F32 = jnp.bfloat16, jnp.float32
C = 256
TILES = 4
A, B = 0, 1
RIGHT, LEFT = 0, 1


def dot(a, b, ca=1, cb=0):
    return lax.dot_general(a, b, (((ca,), (cb,)), ((), ())), preferred_element_type=F32)


def sigmoid(g):
    return 0.5 * jnp.tanh(0.5 * g) + 0.5


def normed(h):
    return (h * lax.rsqrt(jnp.mean(h * h, -1, keepdims=True) + 1e-6)).astype(BF)


def await_bytes(ref, sem):
    pltpu.make_async_copy(ref, ref, sem).wait()


def when(condition):
    return (lambda body: body()) if condition is True else pl.when(condition)


def routes(n):
    far, near = n // 2, n - 1 - n // 2
    hops = {(A, RIGHT): far, (A, LEFT): near, (B, RIGHT): near, (B, LEFT): far}
    number, k = {}, 0
    for (m, d), count in hops.items():
        for hop in range(1, count + 1):
            number[m, d, hop] = k
            k += 1
    return hops, number, k


def dealt(w, n):
    ff = w.shape[-1]
    owned, part = ff // n, C // n
    pieces = [w[:, z * owned + j * part : z * owned + (j + 1) * part] for j in range(ff // C) for z in range(n)]
    return jnp.concatenate(pieces, axis=1)


def gathered_back(w, n):
    ff = w.shape[-1]
    part = C // n
    pieces = [w[:, j * C + z * part : j * C + (z + 1) * part] for z in range(n) for j in range(ff // C)]
    return jnp.concatenate(pieces, axis=1)


def step_kernel(
    n, layers, d_model, ff, tokens, units,
    x_hbm, dy_hbm, wg_hbm, wu_hbm, wd_hbm,
    gg_ref, gu_ref, gd_ref, squares_ref, a_hbm,
    x, a, dy, da, hidden, wgu, wd, dgu, hid, acc, buf, ss, others, raw,
    local_sem, own_sem, ag_recv, ag_send, pair_recv, pair_send, side_recv, side_send, rs_recv, rs_send, sq_recv, sq_send, credit,
):
    me, rep = lax.axis_index("dp"), lax.axis_index("rep")
    core, row = lax.rem(rep, 2), lax.rem(rep // 2, 2)
    partner = {"rep": rep + 1 - 2 * core}
    beside = {"rep": rep + 2 - 4 * row}
    ring = lambda off: lax.rem(me + off + n, n)
    to = {RIGHT: {"dp": ring(1)}, LEFT: {"dp": ring(-1)}}
    sign = {RIGHT: 1, LEFT: -1}
    hops, number, messages = routes(n)
    chunks = ff // C
    rows_gu, rows_d = d_model // n, C // n
    half_gu, half_d = rows_gu // 2, rows_d // 2
    half_w = d_model // 2
    tile = tokens // TILES
    MESH = pl.DeviceIdType.MESH

    barrier = pltpu.get_barrier_semaphore()
    for off in range(1, n):
        pl.semaphore_signal(barrier, inc=1, device_id={"dp": ring(off)}, device_id_type=MESH)
    pl.semaphore_signal(barrier, inc=1, device_id=partner, device_id_type=MESH)
    pl.semaphore_signal(barrier, inc=1, device_id=beside, device_id_type=MESH)
    mine_gu = pl.ds(pl.multiple_of(me * rows_gu, rows_gu), rows_gu)
    mine_d = pl.ds(pl.multiple_of(me * rows_d, rows_d), rows_d)
    own = [(wg_hbm, raw.at[0]), (wu_hbm, raw.at[1])]
    for l in range(layers):
        for c in range(chunks):
            own.append((wd_hbm.at[l, pl.ds(c * rows_d, rows_d)], wd.at[l, c, mine_d]))
    own = [pltpu.make_async_copy(s, t, own_sem.at[i]) for i, (s, t) in enumerate(own)]
    for copy in own:
        copy.start()
    load_x = pltpu.make_async_copy(x_hbm, x, local_sem.at[0])
    load_dy = pltpu.make_async_copy(dy_hbm, dy, local_sem.at[1])
    load_x.start()
    load_dy.start()
    own[0].wait()
    own[1].wait()

    def deal(l):
        for m in range(2):
            block = dealt(raw[m, l].astype(F32), n).astype(BF)
            for c in range(chunks):
                wgu[l, c, mine_gu, pl.ds(m * C, C)] = block[:, c * C : (c + 1) * C]

    deal(0)
    pl.semaphore_wait(barrier, n + 1)
    for copy in own[2:]:
        copy.wait()

    def region(u, owner, first, width):
        l, down, c, count = units[u]
        if down:
            rows = pl.ds(pl.multiple_of(owner * rows_d + core * half_d, half_d), half_d)
            return wd.at[l, pl.ds(c, count), rows, pl.ds(first, width)]
        rows = pl.ds(pl.multiple_of(owner * rows_gu + core * half_gu, half_gu), half_gu)
        return wgu.at[l, pl.ds(c, count), rows, pl.ds(pl.multiple_of(first, 128), width)]

    def piece(u, m, owner):
        if units[u][1]:
            return region(u, owner, m * half_w, half_w)
        return region(u, owner, row * C + m * (C // 2), C // 2)

    def amount(u, both=False):
        l, down, c, count = units[u]
        if down:
            return wd.at[l, pl.ds(c, count), pl.ds(0, messages * half_d // 2), pl.ds(0, 2 * half_w)]
        return wgu.at[l, pl.ds(c, count), pl.ds(0, messages * half_gu // 2), pl.ds(0, 2 * C if both else C)]

    def send(block, send_sem, recv_sem, device):
        pltpu.make_async_remote_copy(
            src_ref=block, dst_ref=block, send_sem=send_sem, recv_sem=recv_sem, device_id=device, device_id_type=MESH
        ).start()

    def gather(u, k):
        for (m, d), count in hops.items():
            if k > count:
                continue
            block = piece(u, m, ring(-sign[d] * k))
            if k:
                await_bytes(block, ag_recv.at[u, number[m, d, k]])
            if k < count:
                send(block, ag_send.at[u], ag_recv.at[u, number[m, d, k + 1]], to[d])
            if k:
                if not units[u][1]:
                    send(block, side_send.at[u], side_recv.at[u], beside)
                send(block, pair_send.at[u], pair_recv.at[u], partner)

    def pass_on(u):
        await_bytes(amount(u), side_recv.at[u])
        for off in range(1, n):
            send(region(u, ring(off), (1 - row) * C, C), pair_send.at[u], pair_recv.at[u], partner)

    def gathered(u):
        await_bytes(amount(u, True), pair_recv.at[u])

    def rs_at(s):
        slot = lax.rem(s, 3)
        return acc.at[slot], buf.at[slot], slot

    def rs_term(total, owner, m):
        cols = pl.ds(m * C, C)
        gu = total[pl.ds(pl.multiple_of(owner * rows_gu, rows_gu), rows_gu), cols]
        down = total[pl.ds(pl.multiple_of(d_model + owner * rows_d, rows_d), rows_d), cols]
        return jnp.concatenate([gu, down], axis=0)

    def rs_step(s, k, wait_credit=None):
        total, slots, slot = rs_at(s)
        if wait_credit is not None:

            @when(wait_credit)
            def _():
                pl.semaphore_wait(credit.at[0], 1)
                pl.semaphore_wait(credit.at[1], 1)

        out = []
        for i, ((m, d), count) in enumerate(hops.items()):
            if k >= count:
                continue
            term = rs_term(total, ring(sign[d] * (count - k)), m)
            if k == 0:
                at = messages + i
            else:
                at = number[m, d, k]
                await_bytes(slots.at[at], rs_recv.at[slot, at])
                term = term + slots[at].astype(F32)
            slots[at] = term.astype(BF)
            out.append((m, d, at))
        for m, d, at in out:
            there = number[m, d, k + 1]
            pltpu.make_async_remote_copy(
                src_ref=slots.at[at], dst_ref=slots.at[there], send_sem=rs_send.at[slot], recv_sem=rs_recv.at[slot, there],
                device_id=to[d], device_id_type=MESH,
            ).start()

    def rs_final(s, l, c, give=None):
        total, slots, slot = rs_at(s)
        for m in (A, B):
            g = rs_term(total, me, m)
            for d in (RIGHT, LEFT):
                at = number[m, d, hops[m, d]]
                await_bytes(slots.at[at], rs_recv.at[slot, at])
                g = g + slots[at].astype(F32)
            g = g.astype(BF)
            (gg_ref, gu_ref)[m][l, :, pl.ds(pl.multiple_of(c * C, C), C)] = g[:rows_gu]
            gd_ref[l, pl.ds(pl.multiple_of(c * rows_d, rows_d), rows_d), pl.ds(m * half_w, half_w)] = g[rows_gu:]
            wide = g.astype(F32)
            ss[...] += wide * wide
        await_bytes(slots.at[pl.ds(0, messages)], rs_send.at[slot])
        if give is not None:

            @when(give)
            def _():
                pl.semaphore_signal(credit.at[0], inc=1, device_id=to[LEFT], device_id_type=MESH)
                pl.semaphore_signal(credit.at[1], inc=1, device_id=to[RIGHT], device_id_type=MESH)

    def tile_rows(t):
        return pl.ds(pl.multiple_of(t * tile, tile), tile)

    def first_norm(lo, hi):
        @pl.loop(lo, hi)
        def _(t):
            r = tile_rows(t)
            a[r] = normed(x[r].astype(F32))

    gather(0, 0)
    gather(1, 0)
    ss[...] = jnp.zeros_like(ss)
    load_x.wait()
    first_norm(0, 2)
    gather(0, 1)
    gather(1, 1)
    gather(2, 0)
    first_norm(2, 4)
    save_a = pltpu.make_async_copy(a, a_hbm, local_sem.at[2])
    save_a.start()
    gather(0, 2)
    gather(1, 2)
    gather(2, 1)
    deal(1)
    da[...] = jnp.zeros_like(da)
    gather(0, 3)
    gather(0, 4)
    gather(1, 3)
    gather(2, 2)
    gather(3, 0)
    load_dy.wait()
    pass_on(0)
    gathered(0)

    before = {
        1: [(1, 4), (2, 3), (3, 1)],
        2: [(2, 4), (3, 2), (4, 0)],
        3: [(3, 3), (4, 1), (5, 0)],
        4: [(3, 4), (4, 2), (5, 1)],
    }
    for c in range(chunks):
        for event in before.get(c, ()):
            gather(*event)
        if c == 1:
            pass_on(1)
            gathered(1)
        if c == 2:
            pass_on(2)
        if c == 3:
            gathered(2)

        @pl.loop(0, TILES)
        def _(t):
            r = tile_rows(t)
            both = dot(a[r], wgu[0, c])
            g, u = both[:, :C], both[:, C:]
            hidden[r, c * C : (c + 1) * C] = (g * sigmoid(g) * u).astype(BF)

    gather(4, 3)
    gather(5, 2)
    gathered(3)
    save_a.wait()
    between = {0: [], 1: [(4, 4), (5, 3)], 2: [(5, 4)], 3: []}
    for t in range(TILES):
        for event in between[t]:
            gather(*event)
        if t == 2:
            pass_on(4)
        r = pl.ds(t * tile, tile)
        out = dot(hidden[r], wd[0].reshape(ff, d_model)).astype(BF)
        h = (x[r].astype(F32) + out.astype(F32)).astype(BF)
        x[r] = h
        a[r] = normed(h.astype(F32))
    for u in (4, 5):
        gathered(u)

    def tile_back(l, c, t, back):
        r = tile_rows(t)
        both = dot(a[r], wgu[l, c])
        g, u = both[:, :C], both[:, C:]
        dh = dot(back[r], wd[l, c], 1, 1).astype(BF).astype(F32)
        s = sigmoid(g)
        silu = g * s
        slope = s + silu * (1.0 - s)
        both = jnp.concatenate([(dh * u * slope).astype(BF), (dh * silu).astype(BF)], axis=1)
        dgu[r] = both
        hid[r] = (silu * u).astype(BF)
        if l == layers - 1:
            da[r] += dot(both, wgu[l, c], 1, 1)

    last = layers - 1

    def layer_back(l, s0, back, early):
        give = lambda s: s <= layers * chunks - 4

        @pl.loop(0, chunks)
        def _(c):
            slot = lax.rem(s0 + c, 3)
            early(c, 0)

            @pl.when(c >= 1)
            def _():
                rs_step(s0 + c - 1, 0, s0 + c - 1 >= 3)

            @pl.when(c >= 2)
            def _():
                rs_step(s0 + c - 2, 2)

            @pl.when(c >= 3)
            def _():
                rs_final(s0 + c - 3, l, c - 3, give(s0 + c - 3))

            tile_back(l, c, 0, back)
            tile_back(l, c, 1, back)
            tile_back(l, c, 2, back)
            tile_back(l, c, 3, back)
            early(c, 1)

            @pl.when(c >= 1)
            def _():
                rs_step(s0 + c - 1, 1)

            @pl.when(c >= 2)
            def _():
                rs_step(s0 + c - 2, 3)

            acc[slot, :d_model] = dot(a[...], dgu[...], 0, 0)
            acc[slot, d_model:] = dot(hid[...], back[...], 0, 0)

    layer_back(last, 0, dy, lambda c, point: None)

    load_a = pltpu.make_async_copy(a_hbm, a, local_sem.at[2])
    load_a.start()
    s = chunks - 1
    rs_step(s, 0, True)
    rs_step(s - 1, 2)
    rs_final(s - 2, last, chunks - 3, True)

    @pl.loop(0, TILES)
    def _(t):
        r = tile_rows(t)
        h = x[r].astype(F32)
        by_a = da[r].astype(BF).astype(F32)
        scale = lax.rsqrt(jnp.mean(h * h, -1, keepdims=True) + 1e-6)
        along = jnp.mean(h * by_a, -1, keepdims=True) * (scale * scale * scale)
        by_h = (by_a * scale - h * along).astype(BF)
        x[r] = (dy[r].astype(F32) + by_h.astype(F32)).astype(BF)

    rs_step(s, 1)
    rs_step(s - 1, 3)
    load_a.wait()

    def early(c, point):
        @pl.when(c == 0)
        def _():
            if point == 0:
                rs_step(s, 2)
                rs_final(s - 1, last, chunks - 2, True)
            else:
                rs_step(s, 3)

        if point == 0:

            @pl.when(c == 1)
            def _():
                rs_final(s, last, chunks - 1, True)

    layer_back(0, chunks, x, early)

    s = layers * chunks - 1
    rs_step(s, 0, True)
    rs_step(s - 1, 2)
    rs_final(s - 2, 0, chunks - 3)
    rs_step(s, 1)
    rs_step(s - 1, 3)
    rs_step(s, 2)
    rs_final(s - 1, 0, chunks - 2)
    rs_step(s, 3)
    rs_final(s, 0, chunks - 1)

    others[me] = jnp.full(others.shape[1:], jnp.sum(ss[...]), F32)
    copies = []
    for off in range(1, n):
        copies.append(
            pltpu.make_async_remote_copy(
                src_ref=others.at[me], dst_ref=others.at[me], send_sem=sq_send.at[off], recv_sem=sq_recv.at[off],
                device_id={"dp": ring(off)}, device_id_type=MESH,
            )
        )
    for copy in copies:
        copy.start()
    for off in range(1, n):
        slot = others.at[ring(-off)]
        await_bytes(slot, sq_recv.at[off])
    squares_ref[...] = jnp.sum(others[...], axis=0)
    for copy in copies:
        copy.wait_send()
    for u in range(len(units)):
        await_bytes(amount(u), ag_send.at[u])
        await_bytes(amount(u, True), pair_send.at[u])
        if not units[u][1]:
            await_bytes(amount(u), side_send.at[u])


def adamw_kernel(n, count, squares, *refs):
    factor = jnp.minimum(1.0, 0.5 * lax.rsqrt(squares[0:1, 0:1] / count + 1e-30))
    gs, ws, ms, vs, new_w, new_m, new_v = (refs[i : i + 3] for i in range(0, 21, 3))
    for i in range(3):
        g = gs[i][0].astype(F32) * factor
        g = (g if i == 2 else gathered_back(g, n))[None]
        m = 0.9 * ms[i][...] + 0.1 * g
        v = 0.95 * vs[i][...] + 0.05 * g * g
        w = ws[i][...].astype(F32)
        new_w[i][...] = (w - 0.02 * (m * lax.rsqrt(v + 1e-8) + 0.1 * w)).astype(BF)
        new_m[i][...] = m
        new_v[i][...] = v


def solution(mesh):
    n = mesh.shape["dp"]

    def step(x, dy, *arrays):
        weights, m, v = (arrays[i : i + 3] for i in (0, 3, 6))
        x, dy = x[0], dy[0]
        tokens, d_model = x.shape
        layers, rows_gu, ff = weights[0].shape
        chunks = ff // C
        messages = 2 * (n - 1)
        hbm = pl.BlockSpec(memory_space=pl.ANY)
        vmem = pl.BlockSpec(memory_space=pltpu.VMEM)
        dma = pltpu.SemaphoreType.DMA
        units = [(0, False, 0, 1), (0, False, 1, 2), (0, False, 3, chunks - 3), (0, True, 0, chunks)]
        units += [(1, False, 0, chunks), (1, True, 0, chunks)]
        gg, gu, gd, squares, _ = pl.pallas_call(
            functools.partial(step_kernel, n, layers, d_model, ff, tokens, units),
            out_shape=[jax.ShapeDtypeStruct(w.shape, BF) for w in weights]
            + [jax.ShapeDtypeStruct((8, 128), F32), jax.ShapeDtypeStruct((tokens, d_model), BF)],
            in_specs=[hbm] * 5,
            out_specs=[vmem] * 4 + [hbm],
            scratch_shapes=[
                pltpu.VMEM((tokens, d_model), BF),
                pltpu.VMEM((tokens, d_model), BF),
                pltpu.VMEM((tokens, d_model), BF),
                pltpu.VMEM((tokens, d_model), F32),
                pltpu.VMEM((tokens, ff), BF),
                pltpu.VMEM((layers, chunks, d_model, 2 * C), BF),
                pltpu.VMEM((layers, chunks, C, d_model), BF),
                pltpu.VMEM((tokens, 2 * C), BF),
                pltpu.VMEM((tokens, C), BF),
                pltpu.VMEM((3, d_model + C, 2 * C), F32),
                pltpu.VMEM((3, messages + 4, rows_gu + C // n, C), BF),
                pltpu.VMEM((rows_gu + C // n, C), F32),
                pltpu.VMEM((n, 8, 128), F32),
                pltpu.VMEM((2,) + weights[0].shape, BF),
                dma((3,)),
                dma((2 + layers * chunks,)),
                dma((len(units), messages)),
                dma((len(units),)),
                dma((len(units),)),
                dma((len(units),)),
                dma((len(units),)),
                dma((len(units),)),
                dma((3, messages)),
                dma((3,)),
                dma((n,)),
                dma((n,)),
                pltpu.SemaphoreType.REGULAR((2,)),
            ],
            compiler_params=pltpu.CompilerParams(collective_id=0, has_side_effects=True, vmem_limit_bytes=67043328),
            name="train_step",
        )(x, dy, *weights)

        cut = 2
        specs = [pl.BlockSpec((1, w.shape[1] // cut, w.shape[2]), lambda l, i: (l, i, 0)) for w in weights]
        out = pl.pallas_call(
            functools.partial(adamw_kernel, n, float(n * sum(w.size for w in weights))),
            grid=(layers, cut),
            out_shape=[jax.ShapeDtypeStruct(w.shape, dtype) for dtype in (BF, F32, F32) for w in weights],
            in_specs=[pl.BlockSpec((8, 128), lambda l, i: (0, 0))] + specs * 4,
            out_specs=specs * 3,
            name="adamw",
        )(squares, gg, gu, gd, *weights, *m, *v)
        return tuple(out)

    states, cut = P(("rep", "dp"), None, None), P(None, "dp", None)
    return jax.shard_map(
        step,
        mesh=mesh,
        in_specs=(states, states) + (cut,) * 9,
        out_specs=(P("rep", "dp", None),) * 9,
        check_vma=False,
    )
```

```python
import functools

import jax
import jax.numpy as jnp
from jax import lax
from jax.experimental import pallas as pl
from jax.experimental.pallas import tpu as pltpu
from jax.sharding import PartitionSpec as P

BF, F32 = jnp.bfloat16, jnp.float32
C = 256
TILES = 4
A, B = 0, 1
RIGHT, LEFT = 0, 1


def dot(a, b, ca=1, cb=0):
    return lax.dot_general(a, b, (((ca,), (cb,)), ((), ())), preferred_element_type=F32)


def sigmoid(g):
    return 0.5 * jnp.tanh(0.5 * g) + 0.5


def normed(h):
    return (h * lax.rsqrt(jnp.mean(h * h, -1, keepdims=True) + 1e-6)).astype(BF)


def await_bytes(ref, sem):
    pltpu.make_async_copy(ref, ref, sem).wait()


def when(condition):
    return (lambda body: body()) if condition is True else pl.when(condition)


def routes(n):
    far, near = n // 2, n - 1 - n // 2
    hops = {(A, RIGHT): far, (A, LEFT): near, (B, RIGHT): near, (B, LEFT): far}
    number, k = {}, 0
    for (m, d), count in hops.items():
        for hop in range(1, count + 1):
            number[m, d, hop] = k
            k += 1
    return hops, number, k


def dealt(w, n):
    ff = w.shape[-1]
    owned, part = ff // n, C // n
    pieces = [w[:, z * owned + j * part : z * owned + (j + 1) * part] for j in range(ff // C) for z in range(n)]
    return jnp.concatenate(pieces, axis=1)


def gathered_back(w, n):
    ff = w.shape[-1]
    part = C // n
    pieces = [w[:, j * C + z * part : j * C + (z + 1) * part] for z in range(n) for j in range(ff // C)]
    return jnp.concatenate(pieces, axis=1)


def step_kernel(
    n, layers, d_model, ff, tokens, units,
    x_hbm, dy_hbm, wg_hbm, wu_hbm, wd_hbm,
    gg_hbm, gu_hbm, gd_hbm, squares_ref, a_hbm,
    x, a, dy, da, hidden, wgu, wd, dgu, hid, acc, buf, ss, others, raw, gg_ref, gu_ref, gd_ref,
    local_sem, own_sem, ag_recv, ag_send, pair_recv, pair_send, side_recv, side_send, rs_recv, rs_last, rs_send, sq_recv, sq_send, credit,
):
    me, rep = lax.axis_index("dp"), lax.axis_index("rep")
    core, row = lax.rem(rep, 2), lax.rem(rep // 2, 2)
    partner = {"rep": rep + 1 - 2 * core}
    beside = {"rep": rep + 2 - 4 * row}
    ring = lambda off: lax.rem(me + off + n, n)
    to = {RIGHT: {"dp": ring(1)}, LEFT: {"dp": ring(-1)}}
    sign = {RIGHT: 1, LEFT: -1}
    hops, number, messages = routes(n)
    chunks = ff // C
    rows_gu, rows_d = d_model // n, C // n
    half_gu, half_d = rows_gu // 2, rows_d // 2
    half_w = d_model // 2
    tile = tokens // TILES
    MESH = pl.DeviceIdType.MESH

    barrier = pltpu.get_barrier_semaphore()
    for off in range(1, n):
        pl.semaphore_signal(barrier, inc=1, device_id={"dp": ring(off)}, device_id_type=MESH)
    pl.semaphore_signal(barrier, inc=1, device_id=partner, device_id_type=MESH)
    pl.semaphore_signal(barrier, inc=1, device_id=beside, device_id_type=MESH)
    mine_gu = pl.ds(pl.multiple_of(me * rows_gu, rows_gu), rows_gu)
    mine_d = pl.ds(pl.multiple_of(me * rows_d, rows_d), rows_d)
    own = [(wg_hbm, raw.at[0]), (wu_hbm, raw.at[1])]
    for l in range(layers):
        for c in range(chunks):
            own.append((wd_hbm.at[l, pl.ds(c * rows_d, rows_d)], wd.at[l, c, mine_d]))
    own = [pltpu.make_async_copy(s, t, own_sem.at[i]) for i, (s, t) in enumerate(own)]
    for copy in own:
        copy.start()
    load_x = pltpu.make_async_copy(x_hbm, x, local_sem.at[0])
    load_dy = pltpu.make_async_copy(dy_hbm, dy, local_sem.at[1])
    load_x.start()
    load_dy.start()
    own[0].wait()
    own[1].wait()

    def deal(l):
        for m in range(2):
            block = dealt(raw[m, l].astype(F32), n).astype(BF)
            for c in range(chunks):
                wgu[l, c, mine_gu, pl.ds(m * C, C)] = block[:, c * C : (c + 1) * C]

    deal(0)
    pl.semaphore_wait(barrier, n + 1)
    for copy in own[2:]:
        copy.wait()

    def region(u, owner, first, width):
        l, down, c, count = units[u]
        if down:
            rows = pl.ds(pl.multiple_of(owner * rows_d + core * half_d, half_d), half_d)
            return wd.at[l, pl.ds(c, count), rows, pl.ds(first, width)]
        rows = pl.ds(pl.multiple_of(owner * rows_gu + core * half_gu, half_gu), half_gu)
        return wgu.at[l, pl.ds(c, count), rows, pl.ds(pl.multiple_of(first, 128), width)]

    def piece(u, m, owner):
        if units[u][1]:
            return region(u, owner, m * half_w, half_w)
        return region(u, owner, row * C + m * (C // 2), C // 2)

    def amount(u, both=False):
        l, down, c, count = units[u]
        if down:
            return wd.at[l, pl.ds(c, count), pl.ds(0, messages * half_d // 2), pl.ds(0, 2 * half_w)]
        return wgu.at[l, pl.ds(c, count), pl.ds(0, messages * half_gu // 2), pl.ds(0, 2 * C if both else C)]

    def send(block, send_sem, recv_sem, device):
        pltpu.make_async_remote_copy(
            src_ref=block, dst_ref=block, send_sem=send_sem, recv_sem=recv_sem, device_id=device, device_id_type=MESH
        ).start()

    def gather(u, k):
        for (m, d), count in hops.items():
            if k > count:
                continue
            block = piece(u, m, ring(-sign[d] * k))
            if k:
                await_bytes(block, ag_recv.at[u, number[m, d, k]])
            if k < count:
                send(block, ag_send.at[u], ag_recv.at[u, number[m, d, k + 1]], to[d])
            if k:
                if not units[u][1]:
                    send(block, side_send.at[u], side_recv.at[u], beside)
                send(block, pair_send.at[u], pair_recv.at[u], partner)

    def straight(u):
        for off in sorted(range(1, n), key=lambda off: -min(off, n - off)):
            send(region(u, me, row * C, C), ag_send.at[u], ag_recv.at[u, off], {"dp": ring(off)})

    def straight_in(u):
        for off in sorted(range(1, n), key=lambda off: min(off, n - off)):
            block = region(u, ring(-off), row * C, C)
            await_bytes(block, ag_recv.at[u, off])
            send(block, side_send.at[u], side_recv.at[u], beside)
            send(block, pair_send.at[u], pair_recv.at[u], partner)

    def pass_on(u):
        await_bytes(amount(u), side_recv.at[u])
        for off in range(1, n):
            send(region(u, ring(off), (1 - row) * C, C), pair_send.at[u], pair_recv.at[u], partner)

    def gathered(u):
        await_bytes(amount(u, True), pair_recv.at[u])

    whole = (0, rows_gu + rows_d)
    parts = ((0, rows_gu), (rows_gu, rows_d))

    def rs_at(s, part):
        slot = lax.rem(s, 3)
        return acc.at[slot], buf.at[slot], slot, rs_recv.at[slot] if part is whole else rs_last.at[parts.index(part)]

    def rs_term(total, owner, m, part):
        cols = pl.ds(m * C, C)
        gu = pl.ds(pl.multiple_of(owner * rows_gu, rows_gu), rows_gu)
        down = pl.ds(pl.multiple_of(d_model + owner * rows_d, rows_d), rows_d)
        if part is whole:
            return jnp.concatenate([total[gu, cols], total[down, cols]], axis=0)
        return total[down if part[0] else gu, cols]

    routes_far = (((A, RIGHT), (B, LEFT)), ((A, LEFT), (B, RIGHT)))

    def rs_step(s, k, wait_credit=None, part=whole, groups=routes_far):
        total, slots, slot, recv = rs_at(s, part)
        rows = pl.ds(*part)
        if wait_credit is not None:

            @when(wait_credit)
            def _():
                pl.semaphore_wait(credit.at[0], 1)
                pl.semaphore_wait(credit.at[1], 1)

        for group in groups:
            out = []
            for i, (m, d) in enumerate(group):
                count = hops[m, d]
                if k >= count:
                    continue
                term = rs_term(total, ring(sign[d] * (count - k)), m, part)
                if k == 0:
                    at = messages + 2 * routes_far.index(group) + i
                else:
                    at = number[m, d, k]
                    await_bytes(slots.at[at, rows], recv.at[at])
                    term = term + slots[at, rows].astype(F32)
                slots[at, rows] = term.astype(BF)
                out.append((m, d, at))
            for m, d, at in out:
                there = number[m, d, k + 1]
                pltpu.make_async_remote_copy(
                    src_ref=slots.at[at, rows], dst_ref=slots.at[there, rows], send_sem=rs_send.at[slot], recv_sem=recv.at[there],
                    device_id=to[d], device_id_type=MESH,
                ).start()

    def rs_final(s, l, c, give=None, last_parts=(whole,)):
        for m in (A, B):
            for part in last_parts:
                total, slots, slot, recv = rs_at(s, part)
                rows = pl.ds(*part)
                g = rs_term(total, me, m, part)
                for d in (RIGHT, LEFT):
                    at = number[m, d, hops[m, d]]
                    await_bytes(slots.at[at, rows], recv.at[at])
                    g = g + slots[at, rows].astype(F32)
                g = g.astype(BF)
                if part[0] == 0:
                    (gg_ref, gu_ref)[m][l, :, pl.ds(pl.multiple_of(c * C, C), C)] = g[:rows_gu]
                if part[0] or part is whole:
                    down = g[rows_gu:] if part is whole else g
                    gd_ref[l, pl.ds(pl.multiple_of(c * rows_d, rows_d), rows_d), pl.ds(m * half_w, half_w)] = down
                wide = g.astype(F32)
                ss[rows] += wide * wide
        await_bytes(slots.at[pl.ds(0, messages)], rs_send.at[slot])
        if give is not None:

            @when(give)
            def _():
                pl.semaphore_signal(credit.at[0], inc=1, device_id=to[LEFT], device_id_type=MESH)
                pl.semaphore_signal(credit.at[1], inc=1, device_id=to[RIGHT], device_id_type=MESH)

    def tile_rows(t):
        return pl.ds(pl.multiple_of(t * tile, tile), tile)

    def first_norm(lo, hi):
        @pl.loop(lo, hi)
        def _(t):
            r = tile_rows(t)
            a[r] = normed(x[r].astype(F32))

    gather(2, 0)
    straight(0)
    straight(1)
    ss[...] = jnp.zeros_like(ss)
    load_x.wait()
    first_norm(0, 2)
    gather(2, 1)
    first_norm(2, 4)
    save_a = pltpu.make_async_copy(a, a_hbm, local_sem.at[2])
    save_a.start()
    straight_in(0)
    gather(3, 0)
    deal(1)
    da[...] = jnp.zeros_like(da)
    gather(2, 2)
    straight_in(1)
    gather(4, 0)
    load_dy.wait()
    pass_on(0)
    gathered(0)

    def ready(*us):
        for u in us:
            gathered(u)

    meanwhile = {
        1: lambda: (gather(2, 3), gather(3, 1)),
        2: lambda: (pass_on(1), gather(5, 0), ready(1)),
        3: lambda: (gather(2, 4), gather(4, 1)),
        4: lambda: (gather(3, 2), pass_on(2), ready(2)),
        5: lambda: gather(5, 1),
        6: lambda: gather(4, 2),
        7: lambda: gather(3, 3),
        8: lambda: gather(5, 2),
        9: lambda: (gather(4, 3), gather(3, 4)),
        10: lambda: (save_a.wait(), ready(3)),
        11: lambda: (gather(4, 4), gather(5, 3)),
        13: lambda: (pass_on(4), gather(5, 4)),
        14: lambda: ready(4, 5),
    }
    for point in range(2 * chunks):
        if point in meanwhile:
            meanwhile[point]()
        c, lo = point // 2, point % 2 * 2

        @pl.loop(lo, lo + 2)
        def _(t):
            r = tile_rows(t)
            both = dot(a[r], wgu[0, c])
            g, u = both[:, :C], both[:, C:]
            hidden[r, c * C : (c + 1) * C] = (g * sigmoid(g) * u).astype(BF)

    for t in range(TILES):
        if 2 * chunks + t in meanwhile:
            meanwhile[2 * chunks + t]()
        r = pl.ds(t * tile, tile)
        out = dot(hidden[r], wd[0].reshape(ff, d_model)).astype(BF)
        h = (x[r].astype(F32) + out.astype(F32)).astype(BF)
        x[r] = h
        a[r] = normed(h.astype(F32))
    meanwhile[2 * chunks + TILES]()

    def tile_back(l, c, t, back):
        r = tile_rows(t)
        both = dot(a[r], wgu[l, c])
        g, u = both[:, :C], both[:, C:]
        dh = dot(back[r], wd[l, c], 1, 1).astype(BF).astype(F32)
        s = sigmoid(g)
        silu = g * s
        slope = s + silu * (1.0 - s)
        both = jnp.concatenate([(dh * u * slope).astype(BF), (dh * silu).astype(BF)], axis=1)
        dgu[r] = both
        hid[r] = (silu * u).astype(BF)

    def add_da(l, c, t):
        if l == layers - 1:
            r = tile_rows(t)
            da[r] += dot(dgu[r], wgu[l, c], 1, 1)

    last = layers - 1

    final_stream = layers * chunks - 1

    def layer_back(l, s0, back, early):
        give = lambda s: s <= final_stream - 3

        @pl.loop(0, chunks)
        def _(c):
            slot = lax.rem(s0 + c, 3)

            def steps(point):
                for (chunk, at), step in early.items():
                    if at == point:
                        pl.when(c == chunk)(step)

            @pl.when(c >= 1)
            def _():
                rs_step(s0 + c - 1, 0, s0 + c - 1 >= 3)

            tile_back(l, c, 0, back)
            tile_back(l, c, 1, back)
            add_da(l, c, 0)
            steps(1)

            @pl.when(c >= 2)
            def _():
                rs_step(s0 + c - 2, 3)

            tile_back(l, c, 2, back)
            add_da(l, c, 1)
            steps(2)

            @pl.when(c >= 1)
            def _():
                rs_step(s0 + c - 1, 1)

            tile_back(l, c, 3, back)
            add_da(l, c, 2)

            @pl.when(c >= 2)
            def _():
                rs_final(s0 + c - 2, l, c - 2, give(s0 + c - 2))

            add_da(l, c, 3)
            acc[slot, :d_model] = dot(a[...], dgu[...], 0, 0)
            steps(4)

            @pl.when(c >= 1)
            def _():
                rs_step(s0 + c - 1, 2)

            acc[slot, d_model:] = dot(hid[...], back[...], 0, 0)

    layer_back(last, 0, dy, {})

    load_a = pltpu.make_async_copy(a_hbm, a, local_sem.at[2])
    load_a.start()

    def norm_back(lo, hi):
        @pl.loop(lo, hi)
        def _(t):
            r = tile_rows(t)
            h = x[r].astype(F32)
            by_a = da[r].astype(BF).astype(F32)
            scale = lax.rsqrt(jnp.mean(h * h, -1, keepdims=True) + 1e-6)
            along = jnp.mean(h * by_a, -1, keepdims=True) * (scale * scale * scale)
            by_h = (by_a * scale - h * along).astype(BF)
            x[r] = (dy[r].astype(F32) + by_h.astype(F32)).astype(BF)

    s = chunks - 1
    rs_step(s, 0, True)
    norm_back(0, 2)
    rs_step(s - 1, 3)
    norm_back(2, 4)
    rs_step(s, 1)
    load_a.wait()

    layer_back(
        0, chunks, x,
        {
            (0, 1): lambda: rs_final(s - 1, last, chunks - 2, True),
            (0, 2): lambda: rs_step(s, 2),
            (0, 4): lambda: rs_step(s, 3),
            (1, 1): lambda: rs_final(s, last, chunks - 1, True),
            (chunks - 1, 4): lambda: rs_step(final_stream, 0, True, parts[0]),
        },
    )

    rs_step(final_stream, 0, None, parts[1])
    rs_step(final_stream - 1, 3)
    for k in range(1, n // 2):
        for group in routes_far:
            for part in parts:
                rs_step(final_stream, k, None, part, (group,))
        if k == 1:
            rs_final(final_stream - 1, 0, chunks - 2)
    rs_final(final_stream, 0, chunks - 1, None, parts)

    others[me] = jnp.full(others.shape[1:], jnp.sum(ss[...]), F32)
    copies = []
    for off in range(1, n):
        copies.append(
            pltpu.make_async_remote_copy(
                src_ref=others.at[me], dst_ref=others.at[me], send_sem=sq_send.at[off], recv_sem=sq_recv.at[off],
                device_id={"dp": ring(off)}, device_id_type=MESH,
            )
        )
    for copy in copies:
        copy.start()
    results = [(gg_ref, gg_hbm), (gu_ref, gu_hbm), (gd_ref, gd_hbm)]
    results = [pltpu.make_async_copy(s, t, local_sem.at[i]) for i, (s, t) in enumerate(results)]
    for copy in results:
        copy.start()
    for off in range(1, n):
        slot = others.at[ring(-off)]
        await_bytes(slot, sq_recv.at[off])
    squares_ref[...] = jnp.sum(others[...], axis=0)
    for copy in copies:
        copy.wait_send()
    for copy in results:
        copy.wait()
    for u in range(len(units)):
        await_bytes(amount(u), ag_send.at[u])
        await_bytes(amount(u, True), pair_send.at[u])
        if not units[u][1]:
            await_bytes(amount(u), side_send.at[u])


def adamw_kernel(n, count, squares, *refs):
    factor = jnp.minimum(1.0, 0.5 * lax.rsqrt(squares[0:1, 0:1] / count + 1e-30))
    gs, ws, ms, vs, new_w, new_m, new_v = (refs[i : i + 3] for i in range(0, 21, 3))
    for i in range(3):
        g = gs[i][0].astype(F32) * factor
        g = (g if i == 2 else gathered_back(g, n))[None]
        m = 0.9 * ms[i][...] + 0.1 * g
        v = 0.95 * vs[i][...] + 0.05 * g * g
        w = ws[i][...].astype(F32)
        new_w[i][...] = (w - 0.02 * (m * lax.rsqrt(v + 1e-8) + 0.1 * w)).astype(BF)
        new_m[i][...] = m
        new_v[i][...] = v


def solution(mesh):
    n = mesh.shape["dp"]

    def step(x, dy, *arrays):
        weights, m, v = (arrays[i : i + 3] for i in (0, 3, 6))
        x, dy = x[0], dy[0]
        tokens, d_model = x.shape
        layers, rows_gu, ff = weights[0].shape
        chunks = ff // C
        messages = 2 * (n - 1)
        hbm = pl.BlockSpec(memory_space=pl.ANY)
        vmem = pl.BlockSpec(memory_space=pltpu.VMEM)
        dma = pltpu.SemaphoreType.DMA
        units = [(0, False, 0, 1), (0, False, 1, 1), (0, False, 2, chunks - 2), (0, True, 0, chunks)]
        units += [(1, False, 0, chunks), (1, True, 0, chunks)]
        gg, gu, gd, squares, _ = pl.pallas_call(
            functools.partial(step_kernel, n, layers, d_model, ff, tokens, units),
            out_shape=[jax.ShapeDtypeStruct(w.shape, BF) for w in weights]
            + [jax.ShapeDtypeStruct((8, 128), F32), jax.ShapeDtypeStruct((tokens, d_model), BF)],
            in_specs=[hbm] * 5,
            out_specs=[hbm] * 3 + [vmem, hbm],
            scratch_shapes=[
                pltpu.VMEM((tokens, d_model), BF),
                pltpu.VMEM((tokens, d_model), BF),
                pltpu.VMEM((tokens, d_model), BF),
                pltpu.VMEM((tokens, d_model), F32),
                pltpu.VMEM((tokens, ff), BF),
                pltpu.VMEM((layers, chunks, d_model, 2 * C), BF),
                pltpu.VMEM((layers, chunks, C, d_model), BF),
                pltpu.VMEM((tokens, 2 * C), BF),
                pltpu.VMEM((tokens, C), BF),
                pltpu.VMEM((3, d_model + C, 2 * C), F32),
                pltpu.VMEM((3, messages + 4, rows_gu + C // n, C), BF),
                pltpu.VMEM((rows_gu + C // n, C), F32),
                pltpu.VMEM((n, 8, 128), F32),
                pltpu.VMEM((2,) + weights[0].shape, BF),
                *(pltpu.VMEM(w.shape, BF) for w in weights),
                dma((3,)),
                dma((2 + layers * chunks,)),
                dma((len(units), messages)),
                dma((len(units),)),
                dma((len(units),)),
                dma((len(units),)),
                dma((len(units),)),
                dma((len(units),)),
                dma((3, messages)),
                dma((2, messages)),
                dma((3,)),
                dma((n,)),
                dma((n,)),
                pltpu.SemaphoreType.REGULAR((2,)),
            ],
            compiler_params=pltpu.CompilerParams(collective_id=0, has_side_effects=True, vmem_limit_bytes=67043328),
            name="train_step",
        )(x, dy, *weights)

        cut = 2
        specs = [pl.BlockSpec((1, w.shape[1] // cut, w.shape[2]), lambda l, i: (l, i, 0)) for w in weights]
        out = pl.pallas_call(
            functools.partial(adamw_kernel, n, float(n * sum(w.size for w in weights))),
            grid=(layers, cut),
            out_shape=[jax.ShapeDtypeStruct(w.shape, dtype) for dtype in (BF, F32, F32) for w in weights],
            in_specs=[pl.BlockSpec((8, 128), lambda l, i: (0, 0))] + specs * 4,
            out_specs=specs * 3,
            name="adamw",
        )(squares, gg, gu, gd, *weights, *m, *v)
        return tuple(out)

    states, cut = P(("rep", "dp"), None, None), P(None, "dp", None)
    return jax.shard_map(
        step,
        mesh=mesh,
        in_specs=(states, states) + (cut,) * 9,
        out_specs=(P("rep", "dp", None),) * 9,
        check_vma=False,
    )
```

```python
import functools

import jax
import jax.numpy as jnp
from jax import lax
from jax.experimental import pallas as pl
from jax.experimental.pallas import tpu as pltpu
from jax.sharding import PartitionSpec as P

BF, F32 = jnp.bfloat16, jnp.float32
C = 256
TILES = 4
A, B = 0, 1
RIGHT, LEFT = 0, 1


def dot(a, b, ca=1, cb=0):
    return lax.dot_general(a, b, (((ca,), (cb,)), ((), ())), preferred_element_type=F32)


def sigmoid(g):
    return 0.5 * jnp.tanh(0.5 * g) + 0.5


def normed(h):
    return (h * lax.rsqrt(jnp.mean(h * h, -1, keepdims=True) + 1e-6)).astype(BF)


def await_bytes(ref, sem):
    pltpu.make_async_copy(ref, ref, sem).wait()


def when(condition):
    return (lambda body: body()) if condition is True else pl.when(condition)


def routes(n):
    far, near = n // 2, n - 1 - n // 2
    hops = {(A, RIGHT): far, (A, LEFT): near, (B, RIGHT): near, (B, LEFT): far}
    number, k = {}, 0
    for (m, d), count in hops.items():
        for hop in range(1, count + 1):
            number[m, d, hop] = k
            k += 1
    return hops, number, k


def dealt(w, n):
    ff = w.shape[-1]
    owned, part = ff // n, C // n
    pieces = [w[:, z * owned + j * part : z * owned + (j + 1) * part] for j in range(ff // C) for z in range(n)]
    return jnp.concatenate(pieces, axis=1)


def gathered_back(w, n):
    ff = w.shape[-1]
    part = C // n
    pieces = [w[:, j * C + z * part : j * C + (z + 1) * part] for z in range(n) for j in range(ff // C)]
    return jnp.concatenate(pieces, axis=1)


def step_kernel(
    n, layers, d_model, ff, tokens, units,
    x_hbm, dy_hbm, wg_hbm, wu_hbm, wd_hbm,
    gg_hbm, gu_hbm, gd_hbm, squares_ref, a_hbm, both_hbm,
    x, a, dy, da, hidden, wgu, wd, dgu, hid, acc, buf, ss, others, raw, gg_ref, gu_ref, gd_ref, stage,
    local_sem, own_sem, ag_recv, ag_send, pair_recv, pair_send, side_recv, side_send, rs_recv, rs_last, rs_send, sq_recv, sq_send, stage_sem, credit,
):
    me, rep = lax.axis_index("dp"), lax.axis_index("rep")
    core, row = lax.rem(rep, 2), lax.rem(rep // 2, 2)
    partner = {"rep": rep + 1 - 2 * core}
    beside = {"rep": rep + 2 - 4 * row}
    ring = lambda off: lax.rem(me + off + n, n)
    to = {RIGHT: {"dp": ring(1)}, LEFT: {"dp": ring(-1)}}
    sign = {RIGHT: 1, LEFT: -1}
    hops, number, messages = routes(n)
    chunks = ff // C
    rows_gu, rows_d = d_model // n, C // n
    half_gu, half_d = rows_gu // 2, rows_d // 2
    half_w = d_model // 2
    tile = tokens // TILES
    MESH = pl.DeviceIdType.MESH

    barrier = pltpu.get_barrier_semaphore()
    for off in range(1, n):
        pl.semaphore_signal(barrier, inc=1, device_id={"dp": ring(off)}, device_id_type=MESH)
    pl.semaphore_signal(barrier, inc=1, device_id=partner, device_id_type=MESH)
    pl.semaphore_signal(barrier, inc=1, device_id=beside, device_id_type=MESH)
    mine_gu = pl.ds(pl.multiple_of(me * rows_gu, rows_gu), rows_gu)
    mine_d = pl.ds(pl.multiple_of(me * rows_d, rows_d), rows_d)
    own = [(wg_hbm, raw.at[0]), (wu_hbm, raw.at[1])]
    for l in range(layers):
        for c in range(chunks):
            own.append((wd_hbm.at[l, pl.ds(c * rows_d, rows_d)], wd.at[l, c, mine_d]))
    own = [pltpu.make_async_copy(s, t, own_sem.at[i]) for i, (s, t) in enumerate(own)]
    for copy in own:
        copy.start()
    load_x = pltpu.make_async_copy(x_hbm, x, local_sem.at[0])
    load_dy = pltpu.make_async_copy(dy_hbm, dy, local_sem.at[1])
    load_x.start()
    load_dy.start()
    own[0].wait()
    own[1].wait()

    def deal(l):
        for m in range(2):
            block = dealt(raw[m, l].astype(F32), n).astype(BF)
            for c in range(chunks):
                wgu[l, c, mine_gu, pl.ds(m * C, C)] = block[:, c * C : (c + 1) * C]

    deal(0)
    pl.semaphore_wait(barrier, n + 1)
    for copy in own[2:]:
        copy.wait()

    def region(u, owner, first, width):
        l, down, c, count = units[u]
        if down:
            rows = pl.ds(pl.multiple_of(owner * rows_d + core * half_d, half_d), half_d)
            return wd.at[l, pl.ds(c, count), rows, pl.ds(first, width)]
        rows = pl.ds(pl.multiple_of(owner * rows_gu + core * half_gu, half_gu), half_gu)
        return wgu.at[l, pl.ds(c, count), rows, pl.ds(pl.multiple_of(first, 128), width)]

    def piece(u, m, owner):
        if units[u][1]:
            return region(u, owner, m * half_w, half_w)
        return region(u, owner, row * C + m * (C // 2), C // 2)

    def amount(u, both=False):
        l, down, c, count = units[u]
        if down:
            return wd.at[l, pl.ds(c, count), pl.ds(0, messages * half_d // 2), pl.ds(0, 2 * half_w)]
        return wgu.at[l, pl.ds(c, count), pl.ds(0, messages * half_gu // 2), pl.ds(0, 2 * C if both else C)]

    def send(block, send_sem, recv_sem, device):
        pltpu.make_async_remote_copy(
            src_ref=block, dst_ref=block, send_sem=send_sem, recv_sem=recv_sem, device_id=device, device_id_type=MESH
        ).start()

    def gather(u, k):
        for (m, d), count in hops.items():
            if k > count:
                continue
            block = piece(u, m, ring(-sign[d] * k))
            if k:
                await_bytes(block, ag_recv.at[u, number[m, d, k]])
            if k < count:
                send(block, ag_send.at[u], ag_recv.at[u, number[m, d, k + 1]], to[d])
            if k:
                if not units[u][1]:
                    send(block, side_send.at[u], side_recv.at[u], beside)
                send(block, pair_send.at[u], pair_recv.at[u], partner)

    def straight(u):
        for off in sorted(range(1, n), key=lambda off: -min(off, n - off)):
            send(region(u, me, row * C, C), ag_send.at[u], ag_recv.at[u, off], {"dp": ring(off)})

    def straight_in(u):
        for off in sorted(range(1, n), key=lambda off: min(off, n - off)):
            block = region(u, ring(-off), row * C, C)
            await_bytes(block, ag_recv.at[u, off])
            send(block, side_send.at[u], side_recv.at[u], beside)
            send(block, pair_send.at[u], pair_recv.at[u], partner)

    def pass_on(u):
        await_bytes(amount(u), side_recv.at[u])
        for off in range(1, n):
            send(region(u, ring(off), (1 - row) * C, C), pair_send.at[u], pair_recv.at[u], partner)

    def gathered(u):
        await_bytes(amount(u, True), pair_recv.at[u])

    whole = (0, rows_gu + rows_d)
    parts = ((0, rows_gu), (rows_gu, rows_d))

    def rs_at(s, part):
        slot = lax.rem(s, 3)
        return acc.at[slot], buf.at[slot], slot, rs_recv.at[slot] if part is whole else rs_last.at[parts.index(part)]

    def rs_term(total, owner, m, part):
        cols = pl.ds(m * C, C)
        gu = pl.ds(pl.multiple_of(owner * rows_gu, rows_gu), rows_gu)
        down = pl.ds(pl.multiple_of(d_model + owner * rows_d, rows_d), rows_d)
        if part is whole:
            return jnp.concatenate([total[gu, cols], total[down, cols]], axis=0)
        return total[down if part[0] else gu, cols]

    routes_far = (((A, RIGHT), (B, LEFT)), ((A, LEFT), (B, RIGHT)))

    def rs_step(s, k, wait_credit=None, part=whole, groups=routes_far):
        total, slots, slot, recv = rs_at(s, part)
        rows = pl.ds(*part)
        if wait_credit is not None:

            @when(wait_credit)
            def _():
                pl.semaphore_wait(credit.at[0], 1)
                pl.semaphore_wait(credit.at[1], 1)

        for group in groups:
            out = []
            for i, (m, d) in enumerate(group):
                count = hops[m, d]
                if k >= count:
                    continue
                term = rs_term(total, ring(sign[d] * (count - k)), m, part)
                if k == 0:
                    at = messages + 2 * routes_far.index(group) + i
                else:
                    at = number[m, d, k]
                    await_bytes(slots.at[at, rows], recv.at[at])
                    term = term + slots[at, rows].astype(F32)
                slots[at, rows] = term.astype(BF)
                out.append((m, d, at))
            for m, d, at in out:
                there = number[m, d, k + 1]
                pltpu.make_async_remote_copy(
                    src_ref=slots.at[at, rows], dst_ref=slots.at[there, rows], send_sem=rs_send.at[slot], recv_sem=recv.at[there],
                    device_id=to[d], device_id_type=MESH,
                ).start()

    def rs_final(s, l, c, give=None, last_parts=(whole,)):
        for m in (A, B):
            for part in last_parts:
                total, slots, slot, recv = rs_at(s, part)
                rows = pl.ds(*part)
                g = rs_term(total, me, m, part)
                for d in (RIGHT, LEFT):
                    at = number[m, d, hops[m, d]]
                    await_bytes(slots.at[at, rows], recv.at[at])
                    g = g + slots[at, rows].astype(F32)
                g = g.astype(BF)
                if part[0] == 0:
                    (gg_ref, gu_ref)[m][l, :, pl.ds(pl.multiple_of(c * C, C), C)] = g[:rows_gu]
                if part[0] or part is whole:
                    down = g[rows_gu:] if part is whole else g
                    gd_ref[l, pl.ds(pl.multiple_of(c * rows_d, rows_d), rows_d), pl.ds(m * half_w, half_w)] = down
                wide = g.astype(F32)
                ss[rows] += wide * wide
        await_bytes(slots.at[pl.ds(0, messages)], rs_send.at[slot])
        if give is not None:

            @when(give)
            def _():
                pl.semaphore_signal(credit.at[0], inc=1, device_id=to[LEFT], device_id_type=MESH)
                pl.semaphore_signal(credit.at[1], inc=1, device_id=to[RIGHT], device_id_type=MESH)

    def tile_rows(t):
        return pl.ds(pl.multiple_of(t * tile, tile), tile)

    def first_norm(lo, hi):
        @pl.loop(lo, hi)
        def _(t):
            r = tile_rows(t)
            a[r] = normed(x[r].astype(F32))

    gather(2, 0)
    straight(0)
    straight(1)
    ss[...] = jnp.zeros_like(ss)
    load_x.wait()
    first_norm(0, 2)
    gather(2, 1)
    first_norm(2, 4)
    save_a = pltpu.make_async_copy(a, a_hbm, local_sem.at[2])
    save_a.start()
    straight_in(0)
    gather(3, 0)
    deal(1)
    da[...] = jnp.zeros_like(da)
    gather(2, 2)
    straight_in(1)
    gather(4, 0)
    load_dy.wait()
    pass_on(0)
    gathered(0)

    def ready(*us):
        for u in us:
            gathered(u)

    meanwhile = {
        1: lambda: (gather(2, 3), gather(3, 1)),
        2: lambda: (pass_on(1), gather(5, 0), ready(1)),
        3: lambda: (gather(2, 4), gather(4, 1)),
        4: lambda: (gather(3, 2), pass_on(2), ready(2)),
        5: lambda: gather(5, 1),
        6: lambda: gather(4, 2),
        7: lambda: gather(3, 3),
        8: lambda: gather(5, 2),
        9: lambda: (gather(4, 3), gather(3, 4)),
        10: lambda: (save_a.wait(), ready(3)),
        11: lambda: (gather(4, 4), gather(5, 3)),
        13: lambda: (pass_on(4), gather(5, 4)),
        14: lambda: ready(4, 5),
    }
    for point in range(2 * chunks):
        if point in meanwhile:
            meanwhile[point]()
        c, lo = point // 2, point % 2 * 2

        @pl.loop(lo, lo + 2)
        def _(t):
            r = tile_rows(t)
            slot = lax.rem(t, 2)

            @pl.when(c * TILES + t >= 2)
            def _():
                await_bytes(stage.at[slot], stage_sem.at[slot])

            both = dot(a[r], wgu[0, c])
            stage[slot] = both
            pltpu.make_async_copy(stage.at[slot], both_hbm.at[c, r], stage_sem.at[slot]).start()
            g, u = both[:, :C], both[:, C:]
            hidden[r, c * C : (c + 1) * C] = (g * sigmoid(g) * u).astype(BF)

    for t in range(TILES):
        if 2 * chunks + t in meanwhile:
            meanwhile[2 * chunks + t]()
        r = pl.ds(t * tile, tile)
        out = dot(hidden[r], wd[0].reshape(ff, d_model)).astype(BF)
        h = (x[r].astype(F32) + out.astype(F32)).astype(BF)
        x[r] = h
        a[r] = normed(h.astype(F32))
    meanwhile[2 * chunks + TILES]()

    for slot in range(2):
        await_bytes(stage.at[slot], stage_sem.at[slot])

    def fetch(c, t):
        pltpu.make_async_copy(both_hbm.at[c, tile_rows(t)], stage.at[t % 2], stage_sem.at[t % 2]).start()

    def tile_back(l, c, t, back):
        r = tile_rows(t)
        if l == layers - 1:
            both = dot(a[r], wgu[l, c])
        else:
            await_bytes(stage.at[t % 2], stage_sem.at[t % 2])
            both = stage[t % 2]
        g, u = both[:, :C], both[:, C:]
        dh = dot(back[r], wd[l, c], 1, 1).astype(BF).astype(F32)
        s = sigmoid(g)
        silu = g * s
        slope = s + silu * (1.0 - s)
        both = jnp.concatenate([(dh * u * slope).astype(BF), (dh * silu).astype(BF)], axis=1)
        dgu[r] = both
        hid[r] = (silu * u).astype(BF)
        if l < layers - 1:
            if t + 2 < TILES:
                fetch(c, t + 2)
            else:
                fetch(lax.rem(c + 1, chunks), t + 2 - TILES)

    def add_da(l, c, t):
        if l == layers - 1:
            r = tile_rows(t)
            da[r] += dot(dgu[r], wgu[l, c], 1, 1)

    last = layers - 1

    final_stream = layers * chunks - 1

    def layer_back(l, s0, back, early):
        give = lambda s: s <= final_stream - 3

        @pl.loop(0, chunks)
        def _(c):
            slot = lax.rem(s0 + c, 3)

            def steps(point):
                for (chunk, at), step in early.items():
                    if at == point:
                        pl.when(c == chunk)(step)

            @pl.when(c >= 1)
            def _():
                rs_step(s0 + c - 1, 0, s0 + c - 1 >= 3)

            tile_back(l, c, 0, back)
            tile_back(l, c, 1, back)
            add_da(l, c, 0)
            steps(1)

            @pl.when(c >= 2)
            def _():
                rs_step(s0 + c - 2, 3)

            tile_back(l, c, 2, back)
            add_da(l, c, 1)
            steps(2)

            @pl.when(c >= 1)
            def _():
                rs_step(s0 + c - 1, 1)

            tile_back(l, c, 3, back)
            add_da(l, c, 2)

            @pl.when(c >= 2)
            def _():
                rs_final(s0 + c - 2, l, c - 2, give(s0 + c - 2))

            add_da(l, c, 3)
            acc[slot, :d_model] = dot(a[...], dgu[...], 0, 0)
            steps(4)

            @pl.when(c >= 1)
            def _():
                rs_step(s0 + c - 1, 2)

            acc[slot, d_model:] = dot(hid[...], back[...], 0, 0)

    layer_back(last, 0, dy, {})

    load_a = pltpu.make_async_copy(a_hbm, a, local_sem.at[2])
    load_a.start()
    fetch(0, 0)
    fetch(0, 1)

    def norm_back(lo, hi):
        @pl.loop(lo, hi)
        def _(t):
            r = tile_rows(t)
            h = x[r].astype(F32)
            by_a = da[r].astype(BF).astype(F32)
            scale = lax.rsqrt(jnp.mean(h * h, -1, keepdims=True) + 1e-6)
            along = jnp.mean(h * by_a, -1, keepdims=True) * (scale * scale * scale)
            by_h = (by_a * scale - h * along).astype(BF)
            x[r] = (dy[r].astype(F32) + by_h.astype(F32)).astype(BF)

    s = chunks - 1
    rs_step(s, 0, True)
    norm_back(0, 2)
    rs_step(s - 1, 3)
    norm_back(2, 4)
    rs_step(s, 1)
    load_a.wait()

    layer_back(
        0, chunks, x,
        {
            (0, 1): lambda: rs_final(s - 1, last, chunks - 2, True),
            (0, 2): lambda: rs_step(s, 2),
            (0, 4): lambda: rs_step(s, 3),
            (1, 1): lambda: rs_final(s, last, chunks - 1, True),
            (chunks - 1, 4): lambda: rs_step(final_stream, 0, True, parts[0]),
        },
    )

    for slot in range(2):
        await_bytes(stage.at[slot], stage_sem.at[slot])

    rs_step(final_stream, 0, None, parts[1])
    rs_step(final_stream - 1, 3)
    for k in range(1, n // 2):
        for group in routes_far:
            for part in parts:
                rs_step(final_stream, k, None, part, (group,))
        if k == 1:
            rs_final(final_stream - 1, 0, chunks - 2)
    rs_final(final_stream, 0, chunks - 1, None, parts)

    others[me] = jnp.full(others.shape[1:], jnp.sum(ss[...]), F32)
    copies = []
    for off in range(1, n):
        copies.append(
            pltpu.make_async_remote_copy(
                src_ref=others.at[me], dst_ref=others.at[me], send_sem=sq_send.at[off], recv_sem=sq_recv.at[off],
                device_id={"dp": ring(off)}, device_id_type=MESH,
            )
        )
    for copy in copies:
        copy.start()
    for l in range(layers):
        for ref in (gg_ref, gu_ref):
            ref[l] = gathered_back(ref[l].astype(F32), n).astype(BF)
    results = [(gg_ref, gg_hbm), (gu_ref, gu_hbm), (gd_ref, gd_hbm)]
    results = [pltpu.make_async_copy(s, t, local_sem.at[i]) for i, (s, t) in enumerate(results)]
    for copy in results:
        copy.start()
    for off in range(1, n):
        slot = others.at[ring(-off)]
        await_bytes(slot, sq_recv.at[off])
    squares_ref[...] = jnp.sum(others[...], axis=0)
    for copy in copies:
        copy.wait_send()
    for copy in results:
        copy.wait()
    for u in range(len(units)):
        await_bytes(amount(u), ag_send.at[u])
        await_bytes(amount(u, True), pair_send.at[u])
        if not units[u][1]:
            await_bytes(amount(u), side_send.at[u])


def adamw_kernel(count, squares, *refs):
    factor = jnp.minimum(1.0, 0.5 * lax.rsqrt(squares[0:1, 0:1] / count + 1e-30))
    gs, ws, ms, vs, new_w, new_m, new_v = (refs[i : i + 3] for i in range(0, 21, 3))
    for i in range(3):
        g = gs[i][...].astype(F32) * factor
        m = 0.9 * ms[i][...] + 0.1 * g
        v = 0.95 * vs[i][...] + 0.05 * g * g
        w = ws[i][...].astype(F32)
        new_w[i][...] = (w - 0.02 * (m * lax.rsqrt(v + 1e-8) + 0.1 * w)).astype(BF)
        new_m[i][...] = m
        new_v[i][...] = v


def solution(mesh):
    n = mesh.shape["dp"]

    def step(x, dy, *arrays):
        weights, m, v = (arrays[i : i + 3] for i in (0, 3, 6))
        x, dy = x[0], dy[0]
        tokens, d_model = x.shape
        layers, rows_gu, ff = weights[0].shape
        chunks = ff // C
        messages = 2 * (n - 1)
        hbm = pl.BlockSpec(memory_space=pl.ANY)
        vmem = pl.BlockSpec(memory_space=pltpu.VMEM)
        dma = pltpu.SemaphoreType.DMA
        units = [(0, False, 0, 1), (0, False, 1, 1), (0, False, 2, chunks - 2), (0, True, 0, chunks)]
        units += [(1, False, 0, chunks), (1, True, 0, chunks)]
        gg, gu, gd, squares, *_ = pl.pallas_call(
            functools.partial(step_kernel, n, layers, d_model, ff, tokens, units),
            out_shape=[jax.ShapeDtypeStruct(w.shape, BF) for w in weights]
            + [jax.ShapeDtypeStruct((8, 128), F32), jax.ShapeDtypeStruct((tokens, d_model), BF)]
            + [jax.ShapeDtypeStruct((chunks, tokens, 2 * C), F32)],
            in_specs=[hbm] * 5,
            out_specs=[hbm] * 3 + [vmem, hbm, hbm],
            scratch_shapes=[
                pltpu.VMEM((tokens, d_model), BF),
                pltpu.VMEM((tokens, d_model), BF),
                pltpu.VMEM((tokens, d_model), BF),
                pltpu.VMEM((tokens, d_model), F32),
                pltpu.VMEM((tokens, ff), BF),
                pltpu.VMEM((layers, chunks, d_model, 2 * C), BF),
                pltpu.VMEM((layers, chunks, C, d_model), BF),
                pltpu.VMEM((tokens, 2 * C), BF),
                pltpu.VMEM((tokens, C), BF),
                pltpu.VMEM((3, d_model + C, 2 * C), F32),
                pltpu.VMEM((3, messages + 4, rows_gu + C // n, C), BF),
                pltpu.VMEM((rows_gu + C // n, C), F32),
                pltpu.VMEM((n, 8, 128), F32),
                pltpu.VMEM((2,) + weights[0].shape, BF),
                *(pltpu.VMEM(w.shape, BF) for w in weights),
                pltpu.VMEM((2, tokens // TILES, 2 * C), F32),
                dma((3,)),
                dma((2 + layers * chunks,)),
                dma((len(units), messages)),
                dma((len(units),)),
                dma((len(units),)),
                dma((len(units),)),
                dma((len(units),)),
                dma((len(units),)),
                dma((3, messages)),
                dma((2, messages)),
                dma((3,)),
                dma((n,)),
                dma((n,)),
                dma((2,)),
                pltpu.SemaphoreType.REGULAR((2,)),
            ],
            compiler_params=pltpu.CompilerParams(collective_id=0, has_side_effects=True, vmem_limit_bytes=67043328),
            name="train_step",
        )(x, dy, *weights)

        cut = 2
        specs = [pl.BlockSpec((1, w.shape[1] // cut, w.shape[2]), lambda l, i: (l, i, 0)) for w in weights]
        out = pl.pallas_call(
            functools.partial(adamw_kernel, float(n * sum(w.size for w in weights))),
            grid=(layers, cut),
            out_shape=[jax.ShapeDtypeStruct(w.shape, dtype) for dtype in (BF, F32, F32) for w in weights],
            in_specs=[pl.BlockSpec((8, 128), lambda l, i: (0, 0))] + specs * 4,
            out_specs=specs * 3,
            name="adamw",
        )(squares, gg, gu, gd, *weights, *m, *v)
        return tuple(out)

    states, cut = P(("rep", "dp"), None, None), P(None, "dp", None)
    return jax.shard_map(
        step,
        mesh=mesh,
        in_specs=(states, states) + (cut,) * 9,
        out_specs=(P("rep", "dp", None),) * 9,
        check_vma=False,
    )
```
